32 devices in a mesh: blocks: 16 (over z, y, x), cross: 2 (over core).
Axes of the slice: x: 2, y: 2, z: 4, core: 2. Of those that a mesh axis runs over, the one named last changes fastest.
Arguments:
- f_home: float32 [1024, 19, 512], P(('blocks', 'cross')), may hold values from -0.5 to 1.5
- levels: int32 [1024], P(('blocks', 'cross')), may hold values from 0 to 1, as said below
- plan: int32 [1024], P(('blocks', 'cross')), may hold values from 0 to 1023, as said below
Outputs:
- f_owner: float32 [1024, 19, 512], P(('blocks', 'cross'))
The draws below stay inside these ranges and needn't reach their ends.
Inputs may be any that keep to these rules, and one draw needn't show every extreme that they name: `levels`: exactly a quarter of the patches, 8 times the number of devices, have level 1. plan is a permutation of the patch numbers. Of the patches in the slots of one device of f_home, at most 2 have owner slots on one device, and in every draw some device sends exactly 2 to one owner; every device's owner slots receive exactly 8 patches of level 1.
All inputs are finite; a program needn't handle non-finite values.
Results may differ from the reference program's by a relative error of at most 0.0001.
Values sent between devices are 32-bit elements; how exact they have to be, the bound alone decides.
A program may use at most 256 MiB of HBM per device.

```python
import jax
import jax.numpy as jnp
from jax import lax

FLOW_PATCHES = 1
SPAN_PATCHES = 4
DEPTH_PATCHES = 8
EDGE = 8
STEPS = 2
CELLS = 512
PATCH_DEV = 32
FINE_DEV = 8
PATCHES = 1024
N_BLOCKS = 16
N_CROSS = 2
DEVICES = 32


VELOCITIES = ((0, 0, 0), (1, 0, 0), (-1, 0, 0), (0, 1, 0), (0, -1, 0), (0, 0, 1), (0, 0, -1), (1, 1, 0), (-1, -1, 0), (1, -1, 0), (-1, 1, 0), (1, 0, 1), (-1, 0, -1), (1, 0, -1), (-1, 0, 1), (0, 1, 1), (0, -1, -1), (0, 1, -1), (0, -1, 1))


WEIGHTS = (1.0 / 3.0,) + (1.0 / 18.0,) * 6 + (1.0 / 36.0,) * 12


def wake_layout(key):
    key_tie = jax.random.fold_in(key, 7)
    key_owner = jax.random.fold_in(key, 8)
    key_slot = jax.random.fold_in(key, 9)
    key_jitter = jax.random.fold_in(key, 10)
    ident = jnp.arange(PATCHES, dtype=jnp.int32)
    home = ident // PATCH_DEV
    local_id = ident % PATCH_DEV
    flow_x = home // N_CROSS * FLOW_PATCHES + local_id // (SPAN_PATCHES * DEPTH_PATCHES)
    span_y = home % N_CROSS * SPAN_PATCHES + local_id // DEPTH_PATCHES % SPAN_PATCHES
    total_x = FLOW_PATCHES * N_BLOCKS
    total_y = SPAN_PATCHES * N_CROSS
    behind = flow_x - total_x // 8
    lateral = jnp.abs(2 * span_y + 1 - total_y)
    jitter = jax.random.randint(key_jitter, (PATCHES,), 0, 3 * total_x)
    score = jnp.where(behind >= 0, 8 * total_x * total_y, 0) - lateral * total_x - jnp.abs(behind - total_x // 4) * total_y + jitter
    ties = jax.random.permutation(key_tie, PATCHES).astype(jnp.int32)
    order = jnp.argsort(-(score * PATCHES + ties))
    fine_mask = jnp.zeros((PATCHES,), jnp.int32).at[order[:PATCHES // 4]].set(1)
    fine_rank = jnp.cumsum(fine_mask) - 1
    coarse_rank = jnp.cumsum(1 - fine_mask) - 1
    home_fine = jnp.sum(fine_mask.reshape(DEVICES, PATCH_DEV), axis=1)
    home_coarse = PATCH_DEV - home_fine
    fine_before = jnp.cumsum(home_fine) - home_fine
    coarse_before = jnp.arange(DEVICES, dtype=jnp.int32) * PATCH_DEV - fine_before
    chosen = jnp.argmax(jnp.where(home_coarse > 0, home_fine, -1))
    offset = (fine_before[chosen] - coarse_before[chosen] - home_coarse[chosen] + 1) % DEVICES
    coarse_total = PATCHES - PATCHES // 4
    coarse_index = (coarse_rank + offset) % coarse_total
    owner_pos = jnp.where(fine_mask == 1, fine_rank % DEVICES, coarse_index % DEVICES)
    slot_rank = jnp.where(fine_mask == 1, fine_rank // DEVICES, FINE_DEV + coarse_index // DEVICES)
    relabel = jax.random.permutation(key_owner, DEVICES).astype(jnp.int32)
    slot_scores = jax.random.randint(key_slot, (DEVICES, PATCH_DEV), 0, 1 << 20) * PATCH_DEV + jnp.arange(PATCH_DEV, dtype=jnp.int32)[None, :]
    shuffle = jnp.argsort(slot_scores, axis=1).astype(jnp.int32)
    plan = relabel[owner_pos] * PATCH_DEV + shuffle[owner_pos, slot_rank]
    return (fine_mask.astype(jnp.int32), plan.astype(jnp.int32))


def draw_levels(key, part):
    return wake_layout(key)[0]


def draw_plan(key, part):
    return wake_layout(key)[1]


def draw_f_home(key, part):
    key_density = jax.random.fold_in(key, 21)
    key_velocity = jax.random.fold_in(key, 22)
    key_jitter = jax.random.fold_in(key, 23)
    density = 1.0 + 0.05 * jax.random.truncated_normal(key_density, -3.0, 3.0, (PATCHES, CELLS), jnp.float32)
    velocity = 0.03 * jax.random.truncated_normal(key_velocity, -3.0, 3.0, (3, PATCHES, CELLS), jnp.float32)
    velocity = velocity.at[0].add(0.05)
    jitter = jax.random.truncated_normal(key_jitter, -3.0, 3.0, (PATCHES, 19, CELLS), jnp.float32)
    speed_sq = velocity[0] * velocity[0] + velocity[1] * velocity[1] + velocity[2] * velocity[2]
    columns = []
    for speed in range(19):
        step_x, step_y, step_z = VELOCITIES[speed]
        along = step_x * velocity[0] + step_y * velocity[1] + step_z * velocity[2]
        columns.append(WEIGHTS[speed] * (density * (1.0 + 3.0 * along + 4.5 * along * along - 1.5 * speed_sq) + 0.3 * jitter[:, speed]))
    return jnp.stack(columns, axis=1).astype(jnp.float32)


def block_scale(rng, shape, split, low, top_value):
    loudness = 1.0
    for dim, shards_of in split:
        steps = jax.random.uniform(jax.random.fold_in(jax.random.fold_in(rng, 6), dim), (shards_of,), jnp.float32, low / len(split), top_value / len(split))
        loudness = loudness * jnp.repeat(jnp.exp(steps), shape[dim] // shards_of).reshape((-1,) + (1,) * (len(shape) - 1 - dim))
    return loudness


def setup_inputs(seed: int = 0) -> dict:
    seeds = jax.random.split(jax.random.key(seed), 4)
    f_home = draw_f_home(jax.random.fold_in(seeds[3], 71), 0)
    levels = draw_levels(jax.random.fold_in(seeds[3], 71), 0)
    plan = draw_plan(jax.random.fold_in(seeds[3], 71), 0)
    return dict(f_home=f_home, levels=levels, plan=plan)


VELOCITIES = ((0, 0, 0), (1, 0, 0), (-1, 0, 0), (0, 1, 0), (0, -1, 0), (0, 0, 1), (0, 0, -1), (1, 1, 0), (-1, -1, 0), (1, -1, 0), (-1, 1, 0), (1, 0, 1), (-1, 0, -1), (1, 0, -1), (-1, 0, 1), (0, 1, 1), (0, -1, -1), (0, 1, -1), (0, -1, 1))
WEIGHTS = (1.0 / 3.0,) + (1.0 / 18.0,) * 6 + (1.0 / 36.0,) * 12
FACE_SPEEDS = ((2, 8, 10, 12, 14), (1, 7, 9, 11, 13), (4, 8, 9, 16, 18), (3, 7, 10, 15, 17), (6, 12, 13, 16, 17), (5, 11, 14, 15, 18))
TAU_COARSE = 0.55
TAU_FINE = 2.0 * TAU_COARSE - 0.5
RESCALE = TAU_FINE / (2.0 * TAU_COARSE)
INFLOW = 0.08


def moments(field):
    density = jnp.sum(field, axis=1)
    velocity = []
    for axis_id in range(3):
        forward = [speed for speed in range(19) if VELOCITIES[speed][axis_id] == 1]
        backward = [speed for speed in range(19) if VELOCITIES[speed][axis_id] == -1]
        velocity.append((jnp.sum(field[:, forward], axis=1) - jnp.sum(field[:, backward], axis=1)) / density)
    return density, velocity


def equilibrium(density, velocity, speeds):
    speed_sq = velocity[0] * velocity[0] + velocity[1] * velocity[1] + velocity[2] * velocity[2]
    columns = []
    for speed in speeds:
        step_x, step_y, step_z = VELOCITIES[speed]
        along = step_x * velocity[0] + step_y * velocity[1] + step_z * velocity[2]
        columns.append(WEIGHTS[speed] * density * (1.0 + 3.0 * along + 4.5 * along * along - 1.5 * speed_sq))
    return jnp.stack(columns, axis=1)


def collide(field, relax_rate):
    density, velocity = moments(field)
    balance = equilibrium(density, velocity, range(19))
    relaxed = field + relax_rate[:, None, None, None, None] * (balance - field)
    return relaxed, balance, density, velocity


def layer(field, face_id):
    layer_at = 0 if face_id % 2 == 0 else field.shape[-1] - 1
    return jnp.take(field, layer_at, axis=2 + face_id // 2)


def face_payload(relaxed, balance, send_scale):
    eq_faces = jnp.stack([layer(balance[:, list(FACE_SPEEDS[face_id])], face_id) for face_id in range(6)], axis=1)
    out_faces = jnp.stack([layer(relaxed[:, list(FACE_SPEEDS[face_id])], face_id) for face_id in range(6)], axis=1)
    return eq_faces, send_scale[:, None, None, None, None] * (out_faces - eq_faces)


def inflow_column(speeds):
    values = []
    for speed in speeds:
        along = VELOCITIES[speed][0] * INFLOW
        values.append(WEIGHTS[speed] * (1.0 + 3.0 * along + 4.5 * along * along - 1.5 * INFLOW * INFLOW))
    return jnp.array(values, jnp.float32)


def framed(center, top_row, bottom_row, left_col, right_col):
    middle = jnp.concatenate([left_col[..., :, None], center, right_col[..., :, None]], axis=-1)
    corner = jnp.zeros(top_row.shape[:-1] + (1,), top_row.dtype)
    upper = jnp.concatenate([corner, top_row, corner], axis=-1)[..., None, :]
    lower = jnp.concatenate([corner, bottom_row, corner], axis=-1)[..., None, :]
    return jnp.concatenate([upper, middle, lower], axis=-2)


def bordered(center, left_col, right_col):
    return jnp.concatenate([left_col[..., None], center, right_col[..., None]], axis=-1)


def assemble(eq_ext, neq_ext, recv_scale, inflow_side, outflow_side):
    size_x, size_y, size_z = recv_scale.shape
    factor = recv_scale[:, :, :, None, None, None]

    def neighbour(shift_x, shift_y, shift_z, face_id):
        window = (slice(1 + shift_x, 1 + shift_x + size_x), slice(1 + shift_y, 1 + shift_y + size_y), slice(1 + shift_z, 1 + shift_z + size_z), face_id)
        return eq_ext[window] + factor * neq_ext[window]

    plane_west = framed(neighbour(-1, 0, 0, 1), neighbour(-1, -1, 0, 1)[..., -1, :], neighbour(-1, 1, 0, 1)[..., 0, :], neighbour(-1, 0, -1, 1)[..., :, -1], neighbour(-1, 0, 1, 1)[..., :, 0])
    plane_east = framed(neighbour(1, 0, 0, 0), neighbour(1, -1, 0, 0)[..., -1, :], neighbour(1, 1, 0, 0)[..., 0, :], neighbour(1, 0, -1, 0)[..., :, -1], neighbour(1, 0, 1, 0)[..., :, 0])
    plane_south = bordered(neighbour(0, -1, 0, 3), neighbour(0, -1, -1, 3)[..., :, -1], neighbour(0, -1, 1, 3)[..., :, 0])
    plane_north = bordered(neighbour(0, 1, 0, 2), neighbour(0, 1, -1, 2)[..., :, -1], neighbour(0, 1, 1, 2)[..., :, 0])
    plane_below = neighbour(0, 0, -1, 5)
    plane_above = neighbour(0, 0, 1, 4)
    plane_west = jnp.where(inflow_side[:, None, None, None, None, None], inflow_column(FACE_SPEEDS[1])[:, None, None], plane_west)
    plane_east = jnp.where(outflow_side[:, None, None, None, None, None], inflow_column(FACE_SPEEDS[0])[:, None, None], plane_east)
    return plane_west, plane_east, plane_south, plane_north, plane_below, plane_above


def propagate(relaxed, planes):
    patch_total = relaxed.shape[0]
    extent = relaxed.shape[-1]
    padded = jnp.zeros((patch_total, 19, extent + 2, extent + 2, extent + 2), relaxed.dtype)
    padded = padded.at[:, :, 1:extent + 1, 1:extent + 1, 1:extent + 1].set(relaxed)
    plane_west, plane_east, plane_south, plane_north, plane_below, plane_above = planes
    for column, speed in enumerate(FACE_SPEEDS[1]):
        padded = padded.at[:, speed, 0, :, :].set(plane_west[:, column])
    for column, speed in enumerate(FACE_SPEEDS[0]):
        padded = padded.at[:, speed, extent + 1, :, :].set(plane_east[:, column])
    for column, speed in enumerate(FACE_SPEEDS[3]):
        padded = padded.at[:, speed, 1:extent + 1, 0, :].set(plane_south[:, column])
    for column, speed in enumerate(FACE_SPEEDS[2]):
        padded = padded.at[:, speed, 1:extent + 1, extent + 1, :].set(plane_north[:, column])
    for column, speed in enumerate(FACE_SPEEDS[5]):
        padded = padded.at[:, speed, 1:extent + 1, 1:extent + 1, 0].set(plane_below[:, column])
    for column, speed in enumerate(FACE_SPEEDS[4]):
        padded = padded.at[:, speed, 1:extent + 1, 1:extent + 1, extent + 1].set(plane_above[:, column])
    shifted = []
    for speed in range(19):
        step_x, step_y, step_z = VELOCITIES[speed]
        shifted.append(padded[:, speed, 1 - step_x:1 - step_x + extent, 1 - step_y:1 - step_y + extent, 1 - step_z:1 - step_z + extent])
    return jnp.stack(shifted, axis=1)


def lattice_order(values):
    trailing = values.shape[1:]
    lattice = values.reshape((N_BLOCKS, N_CROSS, FLOW_PATCHES, SPAN_PATCHES, DEPTH_PATCHES) + trailing)
    lattice = jnp.moveaxis(lattice, 2, 1)
    return lattice.reshape((N_BLOCKS * FLOW_PATCHES, N_CROSS * SPAN_PATCHES, DEPTH_PATCHES) + trailing)


def id_order(lattice):
    trailing = lattice.shape[3:]
    grouped = lattice.reshape((N_BLOCKS, FLOW_PATCHES, N_CROSS, SPAN_PATCHES, DEPTH_PATCHES) + trailing)
    grouped = jnp.moveaxis(grouped, 1, 2)
    return grouped.reshape((PATCHES,) + trailing)


def wrap_axis(values, axis_id):
    length = values.shape[axis_id]
    return jnp.concatenate([lax.slice_in_dim(values, length - 1, length, axis=axis_id), values, lax.slice_in_dim(values, 0, 1, axis=axis_id)], axis=axis_id)


def grouped(values):
    return values.reshape((N_BLOCKS * N_CROSS, PATCH_DEV) + values.shape[1:])


def reference(f_home, levels, plan):
    populations = f_home.reshape(PATCHES, 19, EDGE, EDGE, EDGE)
    fine_mask = levels == 1
    relax_rate = jnp.where(fine_mask, 1.0 / TAU_FINE, 1.0 / TAU_COARSE).astype(jnp.float32)
    send_scale = jnp.where(fine_mask, 1.0 / RESCALE, 1.0).astype(jnp.float32)
    recv_scale = lattice_order(jnp.where(fine_mask, RESCALE, 1.0).astype(jnp.float32))
    span_x = FLOW_PATCHES * N_BLOCKS
    position = jnp.arange(span_x, dtype=jnp.int32)

    def group_faces(pieces):
        relaxed, balance, density, velocity = collide(pieces[0], pieces[1])
        return face_payload(relaxed, balance, pieces[2])

    def group_step(pieces):
        fine_rate = jnp.full((PATCH_DEV,), 1.0 / TAU_FINE, jnp.float32)
        planes = pieces[3:]
        relaxed = collide(pieces[0], pieces[1])[0]
        moved = propagate(relaxed, planes)
        updated = propagate(collide(moved, fine_rate)[0], planes)
        return jnp.where(pieces[2][:, None, None, None, None], updated, moved)

    for round_id in range(STEPS):
        eq_faces, neq_faces = lax.map(group_faces, (grouped(populations), grouped(relax_rate), grouped(send_scale)))
        eq_ext = lattice_order(eq_faces.reshape((PATCHES,) + eq_faces.shape[2:]))
        neq_ext = lattice_order(neq_faces.reshape((PATCHES,) + neq_faces.shape[2:]))
        for axis_id in range(3):
            eq_ext = wrap_axis(eq_ext, axis_id)
            neq_ext = wrap_axis(neq_ext, axis_id)
        planes = assemble(eq_ext, neq_ext, recv_scale, position == 0, position == span_x - 1)
        planes = tuple(grouped(id_order(plane)) for plane in planes)
        populations = lax.map(group_step, (grouped(populations), grouped(relax_rate), grouped(fine_mask)) + planes)
        populations = populations.reshape(PATCHES, 19, EDGE, EDGE, EDGE)
    flattened = populations.reshape(PATCHES, 19, CELLS)
    return jnp.zeros_like(flattened).at[plan].set(flattened)
```

```python
import jax
import jax.numpy as jnp
from jax import lax
from jax.experimental import pallas as pl
from jax.experimental.pallas import tpu as pltpu
from jax.sharding import PartitionSpec as P

SPAN_PATCHES = 4
DEPTH_PATCHES = 8
STEPS = 2
CELLS = 512
VELOCITIES = (
    (0, 0, 0),
    (1, 0, 0),
    (-1, 0, 0),
    (0, 1, 0),
    (0, -1, 0),
    (0, 0, 1),
    (0, 0, -1),
    (1, 1, 0),
    (-1, -1, 0),
    (1, -1, 0),
    (-1, 1, 0),
    (1, 0, 1),
    (-1, 0, -1),
    (1, 0, -1),
    (-1, 0, 1),
    (0, 1, 1),
    (0, -1, -1),
    (0, 1, -1),
    (0, -1, 1),
)
WEIGHTS = (1.0 / 3.0,) + (1.0 / 18.0,) * 6 + (1.0 / 36.0,) * 12
TAU_COARSE = 0.55
TAU_FINE = 2.0 * TAU_COARSE - 0.5
RESCALE = TAU_FINE / (2.0 * TAU_COARSE)
INFLOW = 0.08
MESH = pl.DeviceIdType.MESH
PACK = 40
LANES = 128
TILES = CELLS // LANES
Y_UP = [q for q in range(19) if VELOCITIES[q][1] == 1]
Y_DOWN = [q for q in range(19) if VELOCITIES[q][1] == -1]
X_UP = [q for q in range(19) if VELOCITIES[q][0] == 1]
X_DOWN = [q for q in range(19) if VELOCITIES[q][0] == -1]
AROUND = [(dx, dy) for dx in (-1, 0, 1) for dy in (-1, 0, 1) if (dx, dy) != (0, 0)]


def relax_into(load, store, coef):
    f = [load(q) for q in range(19)]
    rho = f[0]
    for q in range(1, 19):
        rho = rho + f[q]
    inv = 1.0 / rho
    u = []
    for axis in range(3):
        up = [f[q] for q in range(19) if VELOCITIES[q][axis] == 1]
        down = [f[q] for q in range(19) if VELOCITIES[q][axis] == -1]
        total = up[0] - down[0]
        for a, b in zip(up[1:], down[1:]):
            total = total + (a - b)
        u.append(total * inv)
    base = 1.0 - 1.5 * (u[0] * u[0] + u[1] * u[1] + u[2] * u[2])
    scaled = {w: w * rho for w in set(WEIGHTS)}
    for q in range(19):
        along = None
        for axis in range(3):
            e = VELOCITIES[q][axis]
            if e:
                term = u[axis] if e == 1 else -u[axis]
                along = term if along is None else along + term
        poly = base if along is None else base + along * (3.0 + 4.5 * along)
        balance = scaled[WEIGHTS[q]] * poly
        store(q, balance + coef(q) * (f[q] - balance))


def lattice_kernel(nb, nc, sidx, f_ref, lev_ref, meta_ref, out_ref, st, pb, cq, pm, lv, ys, yr, xs, xr,
                   send_sem, recv_sem, lsend, lrecv):
    b = lax.axis_index("blocks")
    c = lax.axis_index("cross")

    def at(dx, dy):
        return (lax.rem(b + dx + nb, nb), lax.rem(c + dy + nc, nc))

    barrier = pltpu.get_barrier_semaphore()
    for dx, dy in AROUND:
        pl.semaphore_signal(barrier, inc=1, device_id=at(dx, dy), device_id_type=MESH)
    pl.semaphore_wait(barrier, len(AROUND))

    level_copies = []
    for n, (dx, dy) in enumerate(AROUND):
        copy = pltpu.make_async_remote_copy(
            src_ref=lev_ref, dst_ref=lv.at[n], send_sem=lsend.at[n], recv_sem=lrecv.at[n],
            device_id=at(-dx, -dy), device_id_type=MESH)
        copy.start()
        level_copies.append(copy)

    for q in range(19):
        for r in range(SPAN_PATCHES):
            st[q, r] = f_ref[r * 8 : r * 8 + 8, q, :]

    for copy in level_copies:
        copy.wait()

    own = lev_ref[...]
    scale = {(0, 0): jnp.where(own > 0.5, RESCALE, 1.0)}
    for n, key in enumerate(AROUND):
        scale[key] = jnp.where(lv[n] > 0.5, RESCALE, 1.0)
    patch_scale = {}
    for dx in (-1, 0, 1):
        patch_scale[dx, 0] = scale[dx, 0]
        patch_scale[dx, 1] = jnp.concatenate([scale[dx, 0][1:], scale[dx, 1][:1]], axis=0)
        patch_scale[dx, -1] = jnp.concatenate([scale[dx, -1][-1:], scale[dx, 0][:-1]], axis=0)
    gain = jnp.where(own > 0.5, (1.0 - 1.0 / TAU_FINE) / RESCALE, 1.0 - 1.0 / TAU_COARSE)

    def target_scale(dx, dy, dz):
        value = patch_scale[dx, dy]
        return pltpu.roll(value, (-dz) % 8, axis=1) if dz else value

    shape = (SPAN_PATCHES, 8, LANES)
    lane = lax.broadcasted_iota(jnp.int32, shape, 2)
    for q in range(1, 19):
        e = VELOCITIES[q]
        kinds = [{}]
        for axis in range(3):
            if e[axis]:
                kinds = [{**k, axis: v} for k in kinds for v in (0, 1)]
        table = [(k, target_scale(*[e[a] * k.get(a, 0) for a in range(3)])) for k in kinds]
        for tile in range(TILES):
            cell = lane + tile * LANES
            coord = (cell // 64, (cell // 8) % 8, cell % 8)
            result = table[0][1]
            for k, value in table[1:]:
                mask = None
                for axis, on in k.items():
                    if on:
                        hit = coord[axis] == (7 if e[axis] == 1 else 0)
                        mask = hit if mask is None else mask & hit
                result = jnp.where(mask, value, result)
            cq[q - 1, :, :, tile * LANES : (tile + 1) * LANES] = gain * result

    full = (SPAN_PATCHES, 8, CELLS)
    cell = lax.broadcasted_iota(jnp.int32, full, 2)
    coord = (cell // 64, (cell // 8) % 8, cell % 8)
    entry = {
        (axis, e): coord[axis] == (0 if e == 1 else 7) for axis in range(3) for e in (1, -1)
    }
    half = lax.broadcasted_iota(jnp.int32, (2, 8, LANES), 2) < 64
    fine = jnp.broadcast_to(own[:, :, :1] > 0.5, full)

    def roll(v, amount):
        return pltpu.roll(v, amount % CELLS, axis=2)

    def step(s, carry):
        def chunk(t, carry):
            r = t // TILES
            lanes = pl.ds(pl.multiple_of(lax.rem(t, TILES) * LANES, LANES), LANES)
            plain = jnp.where(lev_ref[r] > 0.5, 1.0 - 1.0 / TAU_FINE, 1.0 - 1.0 / TAU_COARSE)

            def put(q, value):
                pb[q, r, :, lanes] = value

            relax_into(lambda q: st[q, r, :, lanes], put,
                       lambda q: cq[q - 1, r, :, lanes] if q else plain)
            return carry

        lax.fori_loop(0, SPAN_PATCHES * TILES, chunk, 0)

        for q in range(19):
            e = VELOCITIES[q][2]
            if e:
                v = pb[q]
                wrapped = pltpu.roll(roll(v, e - 8 * e), e % 8, axis=1)
                pb[q] = jnp.where(entry[2, e], wrapped, roll(v, e))
        for n in range(5):
            ys[s, 0, n] = pb[Y_UP[n], SPAN_PATCHES - 1]
            ys[s, 1, n] = pb[Y_DOWN[n], 0]
        y_copies = []
        for way, dy in ((0, 1), (1, -1)):
            copy = pltpu.make_async_remote_copy(
                src_ref=ys.at[s, way], dst_ref=yr.at[s, way], send_sem=send_sem.at[s, way],
                recv_sem=recv_sem.at[s, way], device_id=at(0, dy), device_id_type=MESH)
            copy.start()
            y_copies.append(copy)
        st[0] = pb[0]
        st[5] = pb[5]
        st[6] = pb[6]
        for copy in y_copies:
            copy.wait()
        for way, e, group in ((0, 1, Y_UP), (1, -1, Y_DOWN)):
            for n, q in enumerate(group):
                v = pb[q]
                halo = yr[s, way, n][None]
                if e == 1:
                    moved = jnp.concatenate([halo, v[:-1]], axis=0)
                else:
                    moved = jnp.concatenate([v[1:], halo], axis=0)
                v = jnp.where(entry[1, e], roll(moved, 8 * e - 64 * e), roll(v, 8 * e))
                if VELOCITIES[q][0]:
                    pb[q] = v
                else:
                    st[q] = v
        for way, e, group in ((0, 1, X_UP), (1, -1, X_DOWN)):
            for n, q in enumerate(group):
                v = roll(pb[q], 64 * e)
                pb[q] = v
                edge = v[:, :, :LANES] if e == 1 else v[:, :, CELLS - LANES :]
                turned = pltpu.roll(edge, 64, axis=2)
                if e == 1:
                    xs[s, way, n] = jnp.where(half, edge[:2], turned[2:])
                else:
                    xs[s, way, n] = jnp.where(half, turned[:2], edge[2:])
        x_copies = []
        for way, dx in ((0, 1), (1, -1)):
            copy = pltpu.make_async_remote_copy(
                src_ref=xs.at[s, way], dst_ref=xr.at[s, way], send_sem=send_sem.at[s, 2 + way],
                recv_sem=recv_sem.at[s, 2 + way], device_id=at(dx, 0), device_id_type=MESH)
            copy.start()
            x_copies.append(copy)
        for copy in x_copies:
            copy.wait()
        for way, e, group in ((0, 1, X_UP), (1, -1, X_DOWN)):
            outside = b == (0 if e == 1 else nb - 1)
            for n, q in enumerate(group):
                h = xr[s, way, n]
                turned = pltpu.roll(h, 64, axis=2)
                halo = jnp.concatenate([h, turned] if e == 1 else [turned, h], axis=0)
                along = e * INFLOW
                const = WEIGHTS[q] * (1.0 + 3.0 * along + 4.5 * along * along - 1.5 * INFLOW * INFLOW)
                halo = jnp.where(outside, jnp.full(halo.shape, const, jnp.float32), halo)
                if e == 1:
                    st[q, :, :, LANES:] = pb[q, :, :, LANES:]
                    st[q, :, :, :LANES] = jnp.where(lane < 64, halo, pb[q, :, :, :LANES])
                else:
                    st[q, :, :, : CELLS - LANES] = pb[q, :, :, : CELLS - LANES]
                    st[q, :, :, CELLS - LANES :] = jnp.where(lane >= 64, halo, pb[q, :, :, CELLS - LANES :])

        def again(t, carry):
            r = t // TILES
            lanes = pl.ds(pl.multiple_of(lax.rem(t, TILES) * LANES, LANES), LANES)

            def put(q, value):
                pb[q, r, :, lanes] = value

            relax_into(lambda q: st[q, r, :, lanes], put, lambda q: 1.0 - 1.0 / TAU_FINE)
            return carry

        lax.fori_loop(0, SPAN_PATCHES * TILES, again, 0)
        for q in range(19):
            e = VELOCITIES[q]
            take = fine
            for axis in range(3):
                if e[axis]:
                    take = take & ~entry[axis, e[axis]]
            moved = pb[q]
            if q:
                moved = roll(moved, 64 * e[0] + 8 * e[1] + e[2])
            st[q] = jnp.where(take, moved, st[q])
        return carry

    lax.fori_loop(0, STEPS, step, 0)

    for q in range(19):
        for r in range(SPAN_PATCHES):
            pm[r * 8 : r * 8 + 8, q, :] = st[q, r]

    def fill(d, carry):
        for slot in range(2):
            p = sidx[2 * d + slot]
            out_ref[d, 16 * slot : 16 * slot + 16, :] = pm[p, :16, :]
            out_ref[d, 32 + 4 * slot : 35 + 4 * slot, :] = pm[p, 16:19, :]
            out_ref[d, 35 + 4 * slot, :] = meta_ref[d, slot, :]
        return carry

    lax.fori_loop(0, nb * nc, fill, 0)


def unpack_kernel(ridx, got_ref, out_ref):
    def place(t, carry):
        a = ridx[t]
        src = a // 2
        slot = lax.rem(a, 2)
        out_ref[t, :16, :] = got_ref[src, pl.ds(pl.multiple_of(slot * 16, 16), 16), :]
        tail = got_ref[src, 32:40, :]
        out_ref[t, 16:19, :] = jnp.where(slot == 0, tail[:3], tail[4:7])
        return carry

    lax.fori_loop(0, out_ref.shape[0], place, 0)


def body(nb, nc, f_home, levels, plan):
    devices = nb * nc
    patches = f_home.shape[0]
    target = plan // patches
    order = jnp.arange(patches, dtype=jnp.int32)
    earlier = (target[:, None] == target[None, :]) & (order[None, :] < order[:, None])
    place = 2 * target + jnp.sum(earlier.astype(jnp.int32), axis=1)
    hit = place[None, :] == jnp.arange(2 * devices, dtype=jnp.int32)[:, None]
    sidx = jnp.sum(jnp.where(hit, order[None, :], 0), axis=1)
    slot_of = jnp.sum(jnp.where(hit, plan[None, :] % patches + 1, 0), axis=1) - 1
    meta = jnp.broadcast_to(
        slot_of.astype(jnp.float32).reshape(devices, 2, 1), (devices, 2, CELLS)
    )
    lev = jnp.broadcast_to(
        levels.astype(jnp.float32).reshape(SPAN_PATCHES, DEPTH_PATCHES, 1),
        (SPAN_PATCHES, DEPTH_PATCHES, LANES),
    )
    vmem = pl.BlockSpec(memory_space=pltpu.VMEM)
    smem = pl.BlockSpec(memory_space=pltpu.SMEM)
    state = (19, SPAN_PATCHES, 8, CELLS)
    f32 = jnp.float32
    packed = pl.pallas_call(
        lambda *refs: lattice_kernel(nb, nc, *refs),
        out_shape=jax.ShapeDtypeStruct((devices, PACK, CELLS), f32),
        in_specs=[smem, vmem, vmem, vmem],
        out_specs=vmem,
        scratch_shapes=[
            pltpu.VMEM(state, f32),
            pltpu.VMEM(state, f32),
            pltpu.VMEM((18,) + state[1:], f32),
            pltpu.VMEM((patches, 19, CELLS), f32),
            pltpu.VMEM((len(AROUND), SPAN_PATCHES, 8, LANES), f32),
            pltpu.VMEM((STEPS, 2, 5, 8, CELLS), f32),
            pltpu.VMEM((STEPS, 2, 5, 8, CELLS), f32),
            pltpu.VMEM((STEPS, 2, 5, 2, 8, LANES), f32),
            pltpu.VMEM((STEPS, 2, 5, 2, 8, LANES), f32),
            pltpu.SemaphoreType.DMA((STEPS, 4)),
            pltpu.SemaphoreType.DMA((STEPS, 4)),
            pltpu.SemaphoreType.DMA((len(AROUND),)),
            pltpu.SemaphoreType.DMA((len(AROUND),)),
        ],
        compiler_params=pltpu.CompilerParams(collective_id=0, has_side_effects=True,
                                             vmem_limit_bytes=60 * 1024 * 1024),
    )(sidx, f_home, lev, meta)
    got = lax.all_to_all(packed, ("blocks", "cross"), split_axis=0, concat_axis=0, tiled=True)
    marks = jnp.stack([got[:, 35, 0], got[:, 39, 0]], axis=1).reshape(-1)
    match = marks[None, :] == jnp.arange(patches, dtype=f32)[:, None]
    ridx = jnp.sum(
        jnp.where(match, jnp.arange(2 * devices, dtype=jnp.int32)[None, :], 0), axis=1
    )
    return pl.pallas_call(
        unpack_kernel,
        out_shape=jax.ShapeDtypeStruct((patches, 19, CELLS), f32),
        in_specs=[smem, vmem],
        out_specs=vmem,
        compiler_params=pltpu.CompilerParams(vmem_limit_bytes=40 * 1024 * 1024),
    )(ridx, got)


def solution(mesh):
    nb, nc = mesh.shape["blocks"], mesh.shape["cross"]
    in_specs = (P(("blocks", "cross"), None, None), P(("blocks", "cross")), P(("blocks", "cross")))
    out_specs = P(("blocks", "cross"), None, None)
    return jax.shard_map(
        lambda f, l, p: body(nb, nc, f, l, p),
        mesh=mesh, in_specs=in_specs, out_specs=out_specs, check_vma=False)
```

```python
import jax
import jax.numpy as jnp
from jax import lax
from jax.experimental import pallas as pl
from jax.experimental.pallas import tpu as pltpu
from jax.sharding import PartitionSpec as P

SPAN_PATCHES = 4
DEPTH_PATCHES = 8
STEPS = 2
CELLS = 512
VELOCITIES = (
    (0, 0, 0),
    (1, 0, 0),
    (-1, 0, 0),
    (0, 1, 0),
    (0, -1, 0),
    (0, 0, 1),
    (0, 0, -1),
    (1, 1, 0),
    (-1, -1, 0),
    (1, -1, 0),
    (-1, 1, 0),
    (1, 0, 1),
    (-1, 0, -1),
    (1, 0, -1),
    (-1, 0, 1),
    (0, 1, 1),
    (0, -1, -1),
    (0, 1, -1),
    (0, -1, 1),
)
WEIGHTS = (1.0 / 3.0,) + (1.0 / 18.0,) * 6 + (1.0 / 36.0,) * 12
TAU_COARSE = 0.55
TAU_FINE = 2.0 * TAU_COARSE - 0.5
RESCALE = TAU_FINE / (2.0 * TAU_COARSE)
INFLOW = 0.08
MESH = pl.DeviceIdType.MESH
ROWS = 152
MAIN = 16
TAIL = 3
LANES = 128
TILES = CELLS // LANES
Y_UP = [q for q in range(19) if VELOCITIES[q][1] == 1]
Y_DOWN = [q for q in range(19) if VELOCITIES[q][1] == -1]
X_UP = [q for q in range(19) if VELOCITIES[q][0] == 1]
X_DOWN = [q for q in range(19) if VELOCITIES[q][0] == -1]
AROUND = [(dx, dy) for dx in (-1, 0, 1) for dy in (-1, 0, 1) if (dx, dy) != (0, 0)]


def relax_into(load, store, coef):
    f = [load(q) for q in range(19)]
    rho = f[0]
    for q in range(1, 19):
        rho = rho + f[q]
    inv = 1.0 / rho
    u = []
    for axis in range(3):
        up = [f[q] for q in range(19) if VELOCITIES[q][axis] == 1]
        down = [f[q] for q in range(19) if VELOCITIES[q][axis] == -1]
        total = up[0] - down[0]
        for a, b in zip(up[1:], down[1:]):
            total = total + (a - b)
        u.append(total * inv)
    base = 1.0 - 1.5 * (u[0] * u[0] + u[1] * u[1] + u[2] * u[2])
    scaled = {w: w * rho for w in set(WEIGHTS)}
    for q in range(19):
        along = None
        for axis in range(3):
            e = VELOCITIES[q][axis]
            if e:
                term = u[axis] if e == 1 else -u[axis]
                along = term if along is None else along + term
        poly = base if along is None else base + along * (3.0 + 4.5 * along)
        balance = scaled[WEIGHTS[q]] * poly
        store(q, balance + coef(q) * (f[q] - balance))


def lattice_kernel(nb, nc, sidx, slot_of, level, f_ref, got_ref, mark_ref, st, pb, cq, pm, sent, marks,
                   lev_ref, lv, ys, yr, xs, xr, send_sem, recv_sem, lsend, lrecv, psend, precv,
                   msend, mrecv):
    others = nb * nc - 1
    side = nb * nc // 2
    b = lax.axis_index("blocks")
    c = lax.axis_index("cross")

    def at(dx, dy):
        return (lax.rem(b + dx + nb, nb), lax.rem(c + dy + nc, nc))

    me = b * nc + c
    home_half = me // side
    rank = lax.rem(me, side)

    def peer(k):
        far = (1 - home_half) * side + lax.rem(rank + k, side)
        near = home_half * side + lax.rem(rank + 1 + k, side)
        return jnp.where(k < side, far, near)

    def device(d):
        return (d // nc, lax.rem(d, nc))

    barrier = pltpu.get_barrier_semaphore()

    def greet(k, carry):
        pl.semaphore_signal(barrier, inc=1, device_id=device(peer(k)), device_id_type=MESH)
        return carry

    lax.fori_loop(0, others, greet, 0)

    spot = lax.broadcasted_iota(jnp.int32, (SPAN_PATCHES, 8, LANES), 0) * 8
    spot = spot + lax.broadcasted_iota(jnp.int32, (SPAN_PATCHES, 8, LANES), 1)
    own = jnp.zeros((SPAN_PATCHES, 8, LANES), jnp.float32)
    for p in range(SPAN_PATCHES * 8):
        own = jnp.where(spot == p, level[p].astype(jnp.float32), own)
    lev_ref[...] = own

    def note(d, carry):
        row = lax.broadcasted_iota(jnp.int32, (8, LANES), 0)
        first = slot_of[2 * d].astype(jnp.float32)
        second = slot_of[2 * d + 1].astype(jnp.float32)
        marks[d] = jnp.where(row == 0, first, second)
        return carry

    lax.fori_loop(0, others + 1, note, 0)
    for q in range(19):
        for r in range(SPAN_PATCHES):
            st[q, r] = f_ref[q, r * 8 : r * 8 + 8, :]
    pl.semaphore_wait(barrier, others)

    level_copies = []
    for n, (dx, dy) in enumerate(AROUND):
        copy = pltpu.make_async_remote_copy(
            src_ref=lev_ref, dst_ref=lv.at[n], send_sem=lsend.at[n], recv_sem=lrecv.at[n],
            device_id=at(-dx, -dy), device_id_type=MESH)
        copy.start()
        level_copies.append(copy)

    def mark_copy(k):
        d = peer(k)
        return pltpu.make_async_remote_copy(
            src_ref=marks.at[d], dst_ref=mark_ref.at[me], send_sem=msend.at[k],
            recv_sem=mrecv.at[k], device_id=device(d), device_id_type=MESH)

    def patch_copy(k):
        d = peer(k)
        return pltpu.make_async_remote_copy(
            src_ref=sent.at[d], dst_ref=got_ref.at[me], send_sem=psend.at[k],
            recv_sem=precv.at[k], device_id=device(d), device_id_type=MESH)

    def start_mark(k, carry):
        mark_copy(k).start()
        return carry

    lax.fori_loop(0, others, start_mark, 0)
    mark_ref[me] = marks[me]

    for copy in level_copies:
        copy.wait()

    scale = {(0, 0): jnp.where(own > 0.5, RESCALE, 1.0)}
    for n, key in enumerate(AROUND):
        scale[key] = jnp.where(lv[n] > 0.5, RESCALE, 1.0)
    patch_scale = {}
    for dx in (-1, 0, 1):
        patch_scale[dx, 0] = scale[dx, 0]
        patch_scale[dx, 1] = jnp.concatenate([scale[dx, 0][1:], scale[dx, 1][:1]], axis=0)
        patch_scale[dx, -1] = jnp.concatenate([scale[dx, -1][-1:], scale[dx, 0][:-1]], axis=0)
    gain = jnp.where(own > 0.5, (1.0 - 1.0 / TAU_FINE) / RESCALE, 1.0 - 1.0 / TAU_COARSE)

    def target_scale(dx, dy, dz):
        value = patch_scale[dx, dy]
        return pltpu.roll(value, (-dz) % 8, axis=1) if dz else value

    shape = (SPAN_PATCHES, 8, LANES)
    lane = lax.broadcasted_iota(jnp.int32, shape, 2)
    for q in range(1, 19):
        e = VELOCITIES[q]
        kinds = [{}]
        for axis in range(3):
            if e[axis]:
                kinds = [{**k, axis: v} for k in kinds for v in (0, 1)]
        table = [(k, target_scale(*[e[a] * k.get(a, 0) for a in range(3)])) for k in kinds]
        for tile in range(TILES):
            cell = lane + tile * LANES
            coord = (cell // 64, (cell // 8) % 8, cell % 8)
            result = table[0][1]
            for k, value in table[1:]:
                mask = None
                for axis, on in k.items():
                    if on:
                        hit = coord[axis] == (7 if e[axis] == 1 else 0)
                        mask = hit if mask is None else mask & hit
                result = jnp.where(mask, value, result)
            cq[q - 1, :, :, tile * LANES : (tile + 1) * LANES] = gain * result

    full = (SPAN_PATCHES, 8, CELLS)
    cell = lax.broadcasted_iota(jnp.int32, full, 2)
    coord = (cell // 64, (cell // 8) % 8, cell % 8)
    entry = {
        (axis, e): coord[axis] == (0 if e == 1 else 7) for axis in range(3) for e in (1, -1)
    }
    half = lax.broadcasted_iota(jnp.int32, (2, 8, LANES), 2) < 64
    fine = jnp.broadcast_to(own[:, :, :1] > 0.5, full)

    def roll(v, amount):
        return pltpu.roll(v, amount % CELLS, axis=2)

    def step(s, carry):
        def chunk(t, carry):
            r = t // TILES
            lanes = pl.ds(pl.multiple_of(lax.rem(t, TILES) * LANES, LANES), LANES)
            plain = jnp.where(lev_ref[r] > 0.5, 1.0 - 1.0 / TAU_FINE, 1.0 - 1.0 / TAU_COARSE)

            def put(q, value):
                pb[q, r, :, lanes] = value

            relax_into(lambda q: st[q, r, :, lanes], put,
                       lambda q: cq[q - 1, r, :, lanes] if q else plain)
            return carry

        lax.fori_loop(0, SPAN_PATCHES * TILES, chunk, 0)

        for q in range(19):
            e = VELOCITIES[q][2]
            if e:
                v = pb[q]
                wrapped = pltpu.roll(roll(v, e - 8 * e), e % 8, axis=1)
                pb[q] = jnp.where(entry[2, e], wrapped, roll(v, e))
        for n in range(5):
            ys[s, 0, n] = pb[Y_UP[n], SPAN_PATCHES - 1]
            ys[s, 1, n] = pb[Y_DOWN[n], 0]
        y_copies = []
        for way, dy in ((0, 1), (1, -1)):
            copy = pltpu.make_async_remote_copy(
                src_ref=ys.at[s, way], dst_ref=yr.at[s, way], send_sem=send_sem.at[s, way],
                recv_sem=recv_sem.at[s, way], device_id=at(0, dy), device_id_type=MESH)
            copy.start()
            y_copies.append(copy)
        st[0] = pb[0]
        st[5] = pb[5]
        st[6] = pb[6]
        def shift_x(wanted):
            for way, e, group in ((0, 1, X_UP), (1, -1, X_DOWN)):
                for n, q in enumerate(group):
                    if (VELOCITIES[q][1] != 0) != wanted:
                        continue
                    v = roll(pb[q], 64 * e)
                    pb[q] = v
                    edge = v[:, :, :LANES] if e == 1 else v[:, :, CELLS - LANES :]
                    turned = pltpu.roll(edge, 64, axis=2)
                    if e == 1:
                        xs[s, way, n] = jnp.where(half, edge[:2], turned[2:])
                    else:
                        xs[s, way, n] = jnp.where(half, turned[:2], edge[2:])

        def shift_y(wanted):
            for way, e, group in ((0, 1, Y_UP), (1, -1, Y_DOWN)):
                for n, q in enumerate(group):
                    if (VELOCITIES[q][0] != 0) != wanted:
                        continue
                    v = pb[q]
                    halo = yr[s, way, n][None]
                    if e == 1:
                        moved = jnp.concatenate([halo, v[:-1]], axis=0)
                    else:
                        moved = jnp.concatenate([v[1:], halo], axis=0)
                    v = jnp.where(entry[1, e], roll(moved, 8 * e - 64 * e), roll(v, 8 * e))
                    if wanted:
                        pb[q] = v
                    else:
                        st[q] = v

        shift_x(False)
        for copy in y_copies:
            copy.wait()
        shift_y(True)
        shift_x(True)
        x_copies = []
        for way, dx in ((0, 1), (1, -1)):
            copy = pltpu.make_async_remote_copy(
                src_ref=xs.at[s, way], dst_ref=xr.at[s, way], send_sem=send_sem.at[s, 2 + way],
                recv_sem=recv_sem.at[s, 2 + way], device_id=at(dx, 0), device_id_type=MESH)
            copy.start()
            x_copies.append(copy)
        shift_y(False)
        for copy in x_copies:
            copy.wait()
        for way, e, group in ((0, 1, X_UP), (1, -1, X_DOWN)):
            outside = b == (0 if e == 1 else nb - 1)
            for n, q in enumerate(group):
                h = xr[s, way, n]
                turned = pltpu.roll(h, 64, axis=2)
                halo = jnp.concatenate([h, turned] if e == 1 else [turned, h], axis=0)
                along = e * INFLOW
                const = WEIGHTS[q] * (1.0 + 3.0 * along + 4.5 * along * along - 1.5 * INFLOW * INFLOW)
                halo = jnp.where(outside, jnp.full(halo.shape, const, jnp.float32), halo)
                if e == 1:
                    st[q, :, :, LANES:] = pb[q, :, :, LANES:]
                    st[q, :, :, :LANES] = jnp.where(lane < 64, halo, pb[q, :, :, :LANES])
                else:
                    st[q, :, :, : CELLS - LANES] = pb[q, :, :, : CELLS - LANES]
                    st[q, :, :, CELLS - LANES :] = jnp.where(lane >= 64, halo, pb[q, :, :, CELLS - LANES :])

        def again(t, carry):
            r = t // TILES
            lanes = pl.ds(pl.multiple_of(lax.rem(t, TILES) * LANES, LANES), LANES)

            def put(q, value):
                pb[q, r, :, lanes] = value

            relax_into(lambda q: st[q, r, :, lanes], put, lambda q: 1.0 - 1.0 / TAU_FINE)
            return carry

        lax.fori_loop(0, SPAN_PATCHES * TILES, again, 0)
        for q in range(19):
            e = VELOCITIES[q]
            take = fine
            for axis in range(3):
                if e[axis]:
                    take = take & ~entry[axis, e[axis]]
            moved = pb[q]
            if q:
                moved = roll(moved, 64 * e[0] + 8 * e[1] + e[2])
            st[q] = jnp.where(take, moved, st[q])
        return carry

    lax.fori_loop(0, STEPS, step, 0)

    for q in range(19):
        for r in range(SPAN_PATCHES):
            pm[r * 8 : r * 8 + 8, q, :] = st[q, r]

    def pack(d):
        for slot in range(2):
            p = sidx[2 * d + slot]
            for tile in range(TILES):
                lanes = slice(tile * LANES, (tile + 1) * LANES)
                at_row = slot * TILES + tile
                sent[d, at_row * MAIN : (at_row + 1) * MAIN, :] = pm[p, :MAIN, lanes]
                low = 2 * TILES * MAIN + at_row * TAIL
                sent[d, low : low + TAIL, :] = pm[p, MAIN:, lanes]

    def post(k, carry):
        pack(peer(k))

        @pl.when(k > 0)
        def _():
            patch_copy(k - 1).start()

        return carry

    lax.fori_loop(0, others, post, 0)
    pack(me)
    patch_copy(others - 1).start()
    got_ref[me] = sent[me]

    def finish(k, carry):
        mark_copy(k).wait()
        patch_copy(k).wait()
        return carry

    lax.fori_loop(0, others, finish, 0)


def unpack_kernel(ridx, got_ref, out_ref):
    def place(t, carry):
        a = ridx[t]
        src = a // 2
        slot = lax.rem(a, 2)
        tail = got_ref[src, 2 * TILES * MAIN : ROWS, :]
        for tile in range(TILES):
            lanes = slice(tile * LANES, (tile + 1) * LANES)
            low = pl.multiple_of((slot * TILES + tile) * MAIN, MAIN)
            out_ref[:MAIN, t, lanes] = got_ref[src, pl.ds(low, MAIN), :]
            other = TAIL * (TILES + tile)
            rest = jnp.where(
                slot == 0, tail[TAIL * tile : TAIL * (tile + 1)], tail[other : other + TAIL]
            )
            out_ref[MAIN:, t, lanes] = rest
        return carry

    for t in range(out_ref.shape[1]):
        place(t, 0)


def body(nb, nc, f_home, levels, plan):
    devices = nb * nc
    patches = f_home.shape[0]
    target = plan // patches
    order = jnp.arange(patches, dtype=jnp.int32)
    earlier = (target[:, None] == target[None, :]) & (order[None, :] < order[:, None])
    place = 2 * target + jnp.sum(earlier.astype(jnp.int32), axis=1)
    hit = place[None, :] == jnp.arange(2 * devices, dtype=jnp.int32)[:, None]
    sidx = jnp.sum(jnp.where(hit, order[None, :], 0), axis=1)
    slot_of = jnp.sum(jnp.where(hit, plan[None, :] % patches + 1, 0), axis=1) - 1
    vmem = pl.BlockSpec(memory_space=pltpu.VMEM)
    smem = pl.BlockSpec(memory_space=pltpu.SMEM)
    state = (19, SPAN_PATCHES, 8, CELLS)
    small = (SPAN_PATCHES, 8, LANES)
    f32 = jnp.float32
    dma = pltpu.SemaphoreType.DMA
    got, marks = pl.pallas_call(
        lambda *refs: lattice_kernel(nb, nc, *refs),
        out_shape=(
            jax.ShapeDtypeStruct((devices, ROWS, LANES), f32),
            jax.ShapeDtypeStruct((devices, 8, LANES), f32),
        ),
        in_specs=[smem, smem, smem, vmem],
        out_specs=(vmem, vmem),
        scratch_shapes=[
            pltpu.VMEM(state, f32),
            pltpu.VMEM(state, f32),
            pltpu.VMEM((18,) + state[1:], f32),
            pltpu.VMEM((patches, 19, CELLS), f32),
            pltpu.VMEM((devices, ROWS, LANES), f32),
            pltpu.VMEM((devices, 8, LANES), f32),
            pltpu.VMEM(small, f32),
            pltpu.VMEM((len(AROUND),) + small, f32),
            pltpu.VMEM((STEPS, 2, 5, 8, CELLS), f32),
            pltpu.VMEM((STEPS, 2, 5, 8, CELLS), f32),
            pltpu.VMEM((STEPS, 2, 5, 2, 8, LANES), f32),
            pltpu.VMEM((STEPS, 2, 5, 2, 8, LANES), f32),
            dma((STEPS, 4)),
            dma((STEPS, 4)),
            dma((len(AROUND),)),
            dma((len(AROUND),)),
            dma((devices - 1,)),
            dma((devices - 1,)),
            dma((devices - 1,)),
            dma((devices - 1,)),
        ],
        compiler_params=pltpu.CompilerParams(collective_id=0, has_side_effects=True,
                                             vmem_limit_bytes=60 * 1024 * 1024),
    )(sidx, slot_of, levels, jnp.transpose(f_home, (1, 0, 2)))
    match = marks[:, :2, 0].reshape(-1)[None, :] == jnp.arange(patches, dtype=f32)[:, None]
    ridx = jnp.sum(
        jnp.where(match, jnp.arange(2 * devices, dtype=jnp.int32)[None, :], 0), axis=1
    )
    out = pl.pallas_call(
        unpack_kernel,
        out_shape=jax.ShapeDtypeStruct((19, patches, CELLS), f32),
        in_specs=[smem, vmem],
        out_specs=vmem,
        compiler_params=pltpu.CompilerParams(vmem_limit_bytes=40 * 1024 * 1024),
    )(ridx, got)
    return jnp.transpose(out, (1, 0, 2))


def solution(mesh):
    nb, nc = mesh.shape["blocks"], mesh.shape["cross"]
    in_specs = (P(("blocks", "cross"), None, None), P(("blocks", "cross")), P(("blocks", "cross")))
    out_specs = P(("blocks", "cross"), None, None)
    return jax.shard_map(
        lambda f, l, p: body(nb, nc, f, l, p),
        mesh=mesh, in_specs=in_specs, out_specs=out_specs, check_vma=False)
```

```python
import jax
import jax.numpy as jnp
from jax import lax
from jax.experimental import pallas as pl
from jax.experimental.pallas import tpu as pltpu
from jax.sharding import PartitionSpec as P

SPAN_PATCHES = 4
DEPTH_PATCHES = 8
STEPS = 2
CELLS = 512
VELOCITIES = (
    (0, 0, 0),
    (1, 0, 0),
    (-1, 0, 0),
    (0, 1, 0),
    (0, -1, 0),
    (0, 0, 1),
    (0, 0, -1),
    (1, 1, 0),
    (-1, -1, 0),
    (1, -1, 0),
    (-1, 1, 0),
    (1, 0, 1),
    (-1, 0, -1),
    (1, 0, -1),
    (-1, 0, 1),
    (0, 1, 1),
    (0, -1, -1),
    (0, 1, -1),
    (0, -1, 1),
)
WEIGHTS = (1.0 / 3.0,) + (1.0 / 18.0,) * 6 + (1.0 / 36.0,) * 12
TAU_COARSE = 0.55
TAU_FINE = 2.0 * TAU_COARSE - 0.5
RESCALE = TAU_FINE / (2.0 * TAU_COARSE)
INFLOW = 0.08
MESH = pl.DeviceIdType.MESH
ROWS = 152
MAIN = 16
TAIL = 3
LANES = 128
TILES = CELLS // LANES
Y_UP = [q for q in range(19) if VELOCITIES[q][1] == 1]
Y_DOWN = [q for q in range(19) if VELOCITIES[q][1] == -1]
X_UP = [q for q in range(19) if VELOCITIES[q][0] == 1]
X_DOWN = [q for q in range(19) if VELOCITIES[q][0] == -1]
AROUND = [(dx, dy) for dx in (-1, 0, 1) for dy in (-1, 0, 1) if (dx, dy) != (0, 0)]


def relax_into(load, store, coef):
    f = [load(q) for q in range(19)]
    terms = list(f)
    while len(terms) > 1:
        pairs = [a + b for a, b in zip(terms[::2], terms[1::2])]
        terms = pairs + ([terms[-1]] if len(terms) % 2 else [])
    rho = terms[0]
    inv = 1.0 / rho
    u = []
    for axis in range(3):
        up = [f[q] for q in range(19) if VELOCITIES[q][axis] == 1]
        down = [f[q] for q in range(19) if VELOCITIES[q][axis] == -1]
        d = [a - b for a, b in zip(up, down)]
        u.append((((d[0] + d[1]) + (d[2] + d[3])) + d[4]) * inv)
    base = 1.0 - 1.5 * (u[0] * u[0] + u[1] * u[1] + u[2] * u[2])
    scaled = {w: w * rho for w in set(WEIGHTS)}
    for q in range(19):
        along = None
        for axis in range(3):
            e = VELOCITIES[q][axis]
            if e:
                term = u[axis] if e == 1 else -u[axis]
                along = term if along is None else along + term
        poly = base if along is None else base + along * (3.0 + 4.5 * along)
        balance = scaled[WEIGHTS[q]] * poly
        store(q, balance + coef(q) * (f[q] - balance))


def lattice_kernel(nb, nc, sidx, slot_of, level, f_ref, got_ref, table_ref, st, pb, cq, pm, sent, marks, mark_ref,
                   lev_ref, lv, ys, yr, xs, xr, send_sem, recv_sem, lsend, lrecv, psend, precv,
                   msend, mrecv):
    others = nb * nc - 1
    side = nb * nc // 2
    b = lax.axis_index("blocks")
    c = lax.axis_index("cross")

    def at(dx, dy):
        return (lax.rem(b + dx + nb, nb), lax.rem(c + dy + nc, nc))

    me = b * nc + c
    home_half = me // side
    rank = lax.rem(me, side)

    def peer(k):
        far = (1 - home_half) * side + lax.rem(rank + k, side)
        near = home_half * side + lax.rem(rank + 1 + k, side)
        return jnp.where(k < side, far, near)

    def device(d):
        return (d // nc, lax.rem(d, nc))

    barrier = pltpu.get_barrier_semaphore()

    def greet(k, carry):
        pl.semaphore_signal(barrier, inc=1, device_id=device(peer(k)), device_id_type=MESH)
        return carry

    lax.fori_loop(0, others, greet, 0)

    spot = lax.broadcasted_iota(jnp.int32, (SPAN_PATCHES, 8, LANES), 0) * 8
    spot = spot + lax.broadcasted_iota(jnp.int32, (SPAN_PATCHES, 8, LANES), 1)
    own = jnp.zeros((SPAN_PATCHES, 8, LANES), jnp.float32)
    for p in range(SPAN_PATCHES * 8):
        own = jnp.where(spot == p, level[p].astype(jnp.float32), own)
    lev_ref[...] = own

    def note(d, carry):
        row = lax.broadcasted_iota(jnp.int32, (8, LANES), 0)
        first = slot_of[2 * d].astype(jnp.float32)
        second = slot_of[2 * d + 1].astype(jnp.float32)
        marks[d] = jnp.where(row == 0, first, second)
        return carry

    lax.fori_loop(0, others + 1, note, 0)
    for q in range(19):
        for r in range(SPAN_PATCHES):
            st[q, r] = f_ref[q, r * 8 : r * 8 + 8, :]
    pl.semaphore_wait(barrier, others)

    level_copies = []
    for n, (dx, dy) in enumerate(AROUND):
        copy = pltpu.make_async_remote_copy(
            src_ref=lev_ref, dst_ref=lv.at[n], send_sem=lsend.at[n], recv_sem=lrecv.at[n],
            device_id=at(-dx, -dy), device_id_type=MESH)
        copy.start()
        level_copies.append(copy)

    def mark_copy(k):
        d = peer(k)
        return pltpu.make_async_remote_copy(
            src_ref=marks.at[d], dst_ref=mark_ref.at[me], send_sem=msend.at[k],
            recv_sem=mrecv.at[k], device_id=device(d), device_id_type=MESH)

    def patch_copy(k):
        d = peer(k)
        return pltpu.make_async_remote_copy(
            src_ref=sent.at[d], dst_ref=got_ref.at[me], send_sem=psend.at[k],
            recv_sem=precv.at[k], device_id=device(d), device_id_type=MESH)

    def start_mark(k, carry):
        mark_copy(k).start()
        return carry

    lax.fori_loop(0, others, start_mark, 0)
    mark_ref[me] = marks[me]

    for copy in level_copies:
        copy.wait()

    scale = {(0, 0): jnp.where(own > 0.5, RESCALE, 1.0)}
    for n, key in enumerate(AROUND):
        scale[key] = jnp.where(lv[n] > 0.5, RESCALE, 1.0)
    patch_scale = {}
    for dx in (-1, 0, 1):
        patch_scale[dx, 0] = scale[dx, 0]
        patch_scale[dx, 1] = jnp.concatenate([scale[dx, 0][1:], scale[dx, 1][:1]], axis=0)
        patch_scale[dx, -1] = jnp.concatenate([scale[dx, -1][-1:], scale[dx, 0][:-1]], axis=0)
    gain = jnp.where(own > 0.5, (1.0 - 1.0 / TAU_FINE) / RESCALE, 1.0 - 1.0 / TAU_COARSE)

    def target_scale(dx, dy, dz):
        value = patch_scale[dx, dy]
        return pltpu.roll(value, (-dz) % 8, axis=1) if dz else value

    shape = (SPAN_PATCHES, 8, LANES)
    lane = lax.broadcasted_iota(jnp.int32, shape, 2)
    for q in range(1, 19):
        e = VELOCITIES[q]
        kinds = [{}]
        for axis in range(3):
            if e[axis]:
                kinds = [{**k, axis: v} for k in kinds for v in (0, 1)]
        table = [(k, target_scale(*[e[a] * k.get(a, 0) for a in range(3)])) for k in kinds]
        for tile in range(TILES):
            cell = lane + tile * LANES
            coord = (cell // 64, (cell // 8) % 8, cell % 8)
            result = table[0][1]
            for k, value in table[1:]:
                mask = None
                for axis, on in k.items():
                    if on:
                        hit = coord[axis] == (7 if e[axis] == 1 else 0)
                        mask = hit if mask is None else mask & hit
                result = jnp.where(mask, value, result)
            cq[q - 1, :, :, tile * LANES : (tile + 1) * LANES] = gain * result

    full = (SPAN_PATCHES, 8, CELLS)
    cell = lax.broadcasted_iota(jnp.int32, full, 2)
    coord = (cell // 64, (cell // 8) % 8, cell % 8)
    entry = {
        (axis, e): coord[axis] == (0 if e == 1 else 7) for axis in range(3) for e in (1, -1)
    }
    half = lax.broadcasted_iota(jnp.int32, (2, 8, LANES), 2) < 64
    fine = jnp.broadcast_to(own[:, :, :1] > 0.5, full)

    def roll(v, amount):
        return pltpu.roll(v, amount % CELLS, axis=2)

    def step(s, carry):
        def first(r, tile):
            lanes = slice(tile * LANES, (tile + 1) * LANES)
            plain = jnp.where(lev_ref[r] > 0.5, 1.0 - 1.0 / TAU_FINE, 1.0 - 1.0 / TAU_COARSE)

            def put(q, value):
                pb[q, r, :, lanes] = value

            relax_into(lambda q: st[q, r, :, lanes], put,
                       lambda q: cq[q - 1, r, :, lanes] if q else plain)

        def shift_z(q, rows):
            e = VELOCITIES[q][2]
            if e:
                v = pb[q, rows]
                wrapped = pltpu.roll(roll(v, e - 8 * e), e % 8, axis=1)
                pb[q, rows] = jnp.where(entry[2, e][rows], wrapped, roll(v, e))

        def outer(m, carry):
            for tile in range(TILES):
                first(m * (SPAN_PATCHES - 1), tile)
            return carry

        lax.fori_loop(0, 2, outer, 0)
        for r in (0, SPAN_PATCHES - 1):
            for q in range(19):
                shift_z(q, slice(r, r + 1))
        for n in range(5):
            ys[s, 0, n] = pb[Y_UP[n], SPAN_PATCHES - 1]
            ys[s, 1, n] = pb[Y_DOWN[n], 0]
        y_copies = []
        for way, dy in ((0, 1), (1, -1)):
            copy = pltpu.make_async_remote_copy(
                src_ref=ys.at[s, way], dst_ref=yr.at[s, way], send_sem=send_sem.at[s, way],
                recv_sem=recv_sem.at[s, way], device_id=at(0, dy), device_id_type=MESH)
            copy.start()
            y_copies.append(copy)

        def inner(r, carry):
            for tile in range(TILES):
                first(r, tile)
            return carry

        lax.fori_loop(1, SPAN_PATCHES - 1, inner, 0)
        for q in range(19):
            shift_z(q, slice(1, SPAN_PATCHES - 1))
        st[0] = pb[0]
        st[5] = pb[5]
        st[6] = pb[6]
        def shift_x(wanted):
            for way, e, group in ((0, 1, X_UP), (1, -1, X_DOWN)):
                for n, q in enumerate(group):
                    if (VELOCITIES[q][1] != 0) != wanted:
                        continue
                    v = roll(pb[q], 64 * e)
                    pb[q] = v
                    edge = v[:, :, :LANES] if e == 1 else v[:, :, CELLS - LANES :]
                    turned = pltpu.roll(edge, 64, axis=2)
                    if e == 1:
                        xs[s, way, n] = jnp.where(half, edge[:2], turned[2:])
                    else:
                        xs[s, way, n] = jnp.where(half, turned[:2], edge[2:])

        def shift_y(wanted):
            for way, e, group in ((0, 1, Y_UP), (1, -1, Y_DOWN)):
                for n, q in enumerate(group):
                    if (VELOCITIES[q][0] != 0) != wanted:
                        continue
                    v = pb[q]
                    halo = yr[s, way, n][None]
                    if e == 1:
                        moved = jnp.concatenate([halo, v[:-1]], axis=0)
                    else:
                        moved = jnp.concatenate([v[1:], halo], axis=0)
                    v = jnp.where(entry[1, e], roll(moved, 8 * e - 64 * e), roll(v, 8 * e))
                    if wanted:
                        pb[q] = v
                    else:
                        st[q] = v

        shift_x(False)
        for copy in y_copies:
            copy.wait()
        shift_y(True)
        shift_x(True)
        x_copies = []
        for way, dx in ((0, 1), (1, -1)):
            copy = pltpu.make_async_remote_copy(
                src_ref=xs.at[s, way], dst_ref=xr.at[s, way], send_sem=send_sem.at[s, 2 + way],
                recv_sem=recv_sem.at[s, 2 + way], device_id=at(dx, 0), device_id_type=MESH)
            copy.start()
            x_copies.append(copy)
        shift_y(False)
        for q in X_UP + X_DOWN:
            st[q] = pb[q]

        def again(r, tiles):
            for tile in tiles:
                lanes = slice(tile * LANES, (tile + 1) * LANES)

                def put(q, value):
                    pb[q, r, :, lanes] = value

                relax_into(lambda q: st[q, r, :, lanes], put, lambda q: 1.0 - 1.0 / TAU_FINE)

        def middle(r, carry):
            again(r, range(1, TILES - 1))
            return carry

        lax.fori_loop(0, SPAN_PATCHES, middle, 0)
        for copy in x_copies:
            copy.wait()
        for way, e, group in ((0, 1, X_UP), (1, -1, X_DOWN)):
            outside = b == (0 if e == 1 else nb - 1)
            for n, q in enumerate(group):
                h = xr[s, way, n]
                turned = pltpu.roll(h, 64, axis=2)
                halo = jnp.concatenate([h, turned] if e == 1 else [turned, h], axis=0)
                along = e * INFLOW
                const = WEIGHTS[q] * (1.0 + 3.0 * along + 4.5 * along * along - 1.5 * INFLOW * INFLOW)
                halo = jnp.where(outside, jnp.full(halo.shape, const, jnp.float32), halo)
                if e == 1:
                    st[q, :, :, :LANES] = jnp.where(lane < 64, halo, st[q, :, :, :LANES])
                else:
                    st[q, :, :, CELLS - LANES :] = jnp.where(lane >= 64, halo, st[q, :, :, CELLS - LANES :])

        def ends(r, carry):
            again(r, (0, TILES - 1))
            return carry

        lax.fori_loop(0, SPAN_PATCHES, ends, 0)
        for q in range(19):
            e = VELOCITIES[q]
            take = fine
            for axis in range(3):
                if e[axis]:
                    take = take & ~entry[axis, e[axis]]
            moved = pb[q]
            if q:
                moved = roll(moved, 64 * e[0] + 8 * e[1] + e[2])
            st[q] = jnp.where(take, moved, st[q])
        return carry

    lax.fori_loop(0, STEPS, step, 0)

    for q in range(19):
        for r in range(SPAN_PATCHES):
            pm[r * 8 : r * 8 + 8, q, :] = st[q, r]

    def pack(d):
        for slot in range(2):
            p = sidx[2 * d + slot]
            for tile in range(TILES):
                lanes = slice(tile * LANES, (tile + 1) * LANES)
                at_row = slot * TILES + tile
                sent[d, at_row * MAIN : (at_row + 1) * MAIN, :] = pm[p, :MAIN, lanes]
                low = 2 * TILES * MAIN + at_row * TAIL
                sent[d, low : low + TAIL, :] = pm[p, MAIN:, lanes]

    def post(k, carry):
        pack(peer(k))

        @pl.when(k > 0)
        def _():
            patch_copy(k - 1).start()

        return carry

    lax.fori_loop(0, others, post, 0)
    pack(me)
    patch_copy(others - 1).start()
    got_ref[me] = sent[me]

    def marked(k, carry):
        mark_copy(k).wait()
        return carry

    lax.fori_loop(0, others, marked, 0)
    source = lax.broadcasted_iota(jnp.int32, (others + 1, LANES), 0) * 2
    wanted = lax.broadcasted_iota(jnp.int32, (others + 1, LANES), 1).astype(jnp.float32)
    index = jnp.where(mark_ref[:, 0, :] == wanted, source, 0)
    index = index + jnp.where(mark_ref[:, 1, :] == wanted, source + 1, 0)
    table_ref[...] = jnp.broadcast_to(jnp.sum(index, axis=0, keepdims=True), (8, LANES))

    def finish(k, carry):
        patch_copy(k).wait()
        return carry

    lax.fori_loop(0, others, finish, 0)


def unpack_kernel(ridx, got_ref, out_ref):
    def place(t, carry):
        a = ridx[0, t]
        src = a // 2
        slot = lax.rem(a, 2)
        tail = got_ref[src, 2 * TILES * MAIN : ROWS, :]
        for tile in range(TILES):
            lanes = slice(tile * LANES, (tile + 1) * LANES)
            low = pl.multiple_of((slot * TILES + tile) * MAIN, MAIN)
            out_ref[:MAIN, t, lanes] = got_ref[src, pl.ds(low, MAIN), :]
            other = TAIL * (TILES + tile)
            rest = jnp.where(
                slot == 0, tail[TAIL * tile : TAIL * (tile + 1)], tail[other : other + TAIL]
            )
            out_ref[MAIN:, t, lanes] = rest
        return carry

    for t in range(out_ref.shape[1]):
        place(t, 0)


def body(nb, nc, f_home, levels, plan):
    devices = nb * nc
    patches = f_home.shape[0]
    target = plan // patches
    order = jnp.arange(patches, dtype=jnp.int32)
    earlier = (target[:, None] == target[None, :]) & (order[None, :] < order[:, None])
    place = 2 * target + jnp.sum(earlier.astype(jnp.int32), axis=1)
    hit = place[None, :] == jnp.arange(2 * devices, dtype=jnp.int32)[:, None]
    sidx = jnp.sum(jnp.where(hit, order[None, :], 0), axis=1)
    slot_of = jnp.sum(jnp.where(hit, plan[None, :] % patches + 1, 0), axis=1) - 1
    vmem = pl.BlockSpec(memory_space=pltpu.VMEM)
    smem = pl.BlockSpec(memory_space=pltpu.SMEM)
    state = (19, SPAN_PATCHES, 8, CELLS)
    small = (SPAN_PATCHES, 8, LANES)
    f32 = jnp.float32
    dma = pltpu.SemaphoreType.DMA
    got, ridx = pl.pallas_call(
        lambda *refs: lattice_kernel(nb, nc, *refs),
        out_shape=(
            jax.ShapeDtypeStruct((devices, ROWS, LANES), f32),
            jax.ShapeDtypeStruct((8, LANES), jnp.int32),
        ),
        in_specs=[smem, smem, smem, vmem],
        out_specs=(vmem, vmem),
        scratch_shapes=[
            pltpu.VMEM(state, f32),
            pltpu.VMEM(state, f32),
            pltpu.VMEM((18,) + state[1:], f32),
            pltpu.VMEM((patches, 19, CELLS), f32),
            pltpu.VMEM((devices, ROWS, LANES), f32),
            pltpu.VMEM((devices, 8, LANES), f32),
            pltpu.VMEM((devices, 8, LANES), f32),
            pltpu.VMEM(small, f32),
            pltpu.VMEM((len(AROUND),) + small, f32),
            pltpu.VMEM((STEPS, 2, 5, 8, CELLS), f32),
            pltpu.VMEM((STEPS, 2, 5, 8, CELLS), f32),
            pltpu.VMEM((STEPS, 2, 5, 2, 8, LANES), f32),
            pltpu.VMEM((STEPS, 2, 5, 2, 8, LANES), f32),
            dma((STEPS, 4)),
            dma((STEPS, 4)),
            dma((len(AROUND),)),
            dma((len(AROUND),)),
            dma((devices - 1,)),
            dma((devices - 1,)),
            dma((devices - 1,)),
            dma((devices - 1,)),
        ],
        compiler_params=pltpu.CompilerParams(collective_id=0, has_side_effects=True,
                                             vmem_limit_bytes=60 * 1024 * 1024),
    )(sidx, slot_of, levels, jnp.transpose(f_home, (1, 0, 2)))
    out = pl.pallas_call(
        unpack_kernel,
        out_shape=jax.ShapeDtypeStruct((19, patches, CELLS), f32),
        in_specs=[smem, vmem],
        out_specs=vmem,
        compiler_params=pltpu.CompilerParams(vmem_limit_bytes=40 * 1024 * 1024),
    )(ridx, got)
    return jnp.transpose(out, (1, 0, 2))


def solution(mesh):
    nb, nc = mesh.shape["blocks"], mesh.shape["cross"]
    in_specs = (P(("blocks", "cross"), None, None), P(("blocks", "cross")), P(("blocks", "cross")))
    out_specs = P(("blocks", "cross"), None, None)
    return jax.shard_map(
        lambda f, l, p: body(nb, nc, f, l, p),
        mesh=mesh, in_specs=in_specs, out_specs=out_specs, check_vma=False)
```

```python
import jax
import jax.numpy as jnp
from jax import lax
from jax.experimental import pallas as pl
from jax.experimental.pallas import tpu as pltpu
from jax.sharding import PartitionSpec as P

SPAN_PATCHES = 4
DEPTH_PATCHES = 8
STEPS = 2
CELLS = 512
VELOCITIES = (
    (0, 0, 0),
    (1, 0, 0),
    (-1, 0, 0),
    (0, 1, 0),
    (0, -1, 0),
    (0, 0, 1),
    (0, 0, -1),
    (1, 1, 0),
    (-1, -1, 0),
    (1, -1, 0),
    (-1, 1, 0),
    (1, 0, 1),
    (-1, 0, -1),
    (1, 0, -1),
    (-1, 0, 1),
    (0, 1, 1),
    (0, -1, -1),
    (0, 1, -1),
    (0, -1, 1),
)
WEIGHTS = (1.0 / 3.0,) + (1.0 / 18.0,) * 6 + (1.0 / 36.0,) * 12
TAU_COARSE = 0.55
TAU_FINE = 2.0 * TAU_COARSE - 0.5
RESCALE = TAU_FINE / (2.0 * TAU_COARSE)
INFLOW = 0.08
MESH = pl.DeviceIdType.MESH
ROWS = 152
MAIN = 16
TAIL = 3
LANES = 128
TILES = CELLS // LANES
Y_UP = [q for q in range(19) if VELOCITIES[q][1] == 1]
Y_DOWN = [q for q in range(19) if VELOCITIES[q][1] == -1]
X_UP = [q for q in range(19) if VELOCITIES[q][0] == 1]
X_DOWN = [q for q in range(19) if VELOCITIES[q][0] == -1]
AROUND = [(dx, dy) for dx in (-1, 0, 1) for dy in (-1, 0, 1) if (dx, dy) != (0, 0)]


def relax_into(load, store, coef):
    f = [load(q) for q in range(19)]
    terms = list(f)
    while len(terms) > 1:
        pairs = [a + b for a, b in zip(terms[::2], terms[1::2])]
        terms = pairs + ([terms[-1]] if len(terms) % 2 else [])
    rho = terms[0]
    inv = 1.0 / rho
    u = []
    for axis in range(3):
        up = [f[q] for q in range(19) if VELOCITIES[q][axis] == 1]
        down = [f[q] for q in range(19) if VELOCITIES[q][axis] == -1]
        d = [a - b for a, b in zip(up, down)]
        u.append((((d[0] + d[1]) + (d[2] + d[3])) + d[4]) * inv)
    base = 1.0 - 1.5 * (u[0] * u[0] + u[1] * u[1] + u[2] * u[2])
    scaled = {w: w * rho for w in set(WEIGHTS)}
    for q in range(19):
        along = None
        for axis in range(3):
            e = VELOCITIES[q][axis]
            if e:
                term = u[axis] if e == 1 else -u[axis]
                along = term if along is None else along + term
        poly = base if along is None else base + along * (3.0 + 4.5 * along)
        balance = scaled[WEIGHTS[q]] * poly
        store(q, balance + coef(q) * (f[q] - balance))


def lattice_kernel(nb, nc, sidx, slot_of, level, f_ref, got_ref, table_ref, st, pb, cq, pm, sent, marks, mark_ref,
                   lev_ref, lv, ys, yr, xs, xr, send_sem, recv_sem, lsend, lrecv, psend, precv,
                   msend, mrecv):
    others = nb * nc - 1
    side = nb * nc // 2
    b = lax.axis_index("blocks")
    c = lax.axis_index("cross")

    def at(dx, dy):
        return (lax.rem(b + dx + nb, nb), lax.rem(c + dy + nc, nc))

    me = b * nc + c
    home_half = me // side
    rank = lax.rem(me, side)

    def peer(k):
        far = (1 - home_half) * side + lax.rem(rank + k, side)
        near = home_half * side + lax.rem(rank + 1 + k, side)
        return jnp.where(k < side, far, near)

    def device(d):
        return (d // nc, lax.rem(d, nc))

    barrier = pltpu.get_barrier_semaphore()

    def greet(k, carry):
        pl.semaphore_signal(barrier, inc=1, device_id=device(peer(k)), device_id_type=MESH)
        return carry

    lax.fori_loop(0, others, greet, 0)

    spot = lax.broadcasted_iota(jnp.int32, (SPAN_PATCHES, 8, LANES), 0) * 8
    spot = spot + lax.broadcasted_iota(jnp.int32, (SPAN_PATCHES, 8, LANES), 1)
    own = jnp.zeros((SPAN_PATCHES, 8, LANES), jnp.float32)
    for p in range(SPAN_PATCHES * 8):
        own = jnp.where(spot == p, level[p].astype(jnp.float32), own)
    lev_ref[...] = own

    pl.semaphore_wait(barrier, others)

    level_copies = []
    for n, (dx, dy) in enumerate(AROUND):
        copy = pltpu.make_async_remote_copy(
            src_ref=lev_ref, dst_ref=lv.at[n], send_sem=lsend.at[n], recv_sem=lrecv.at[n],
            device_id=at(-dx, -dy), device_id_type=MESH)
        copy.start()
        level_copies.append(copy)

    def note(d, carry):
        row = lax.broadcasted_iota(jnp.int32, (8, LANES), 0)
        first = slot_of[2 * d].astype(jnp.float32)
        second = slot_of[2 * d + 1].astype(jnp.float32)
        marks[d] = jnp.where(row == 0, first, second)
        return carry

    lax.fori_loop(0, others + 1, note, 0)
    for q in range(19):
        for r in range(SPAN_PATCHES):
            st[q, r] = f_ref[q, r * 8 : r * 8 + 8, :]
    def mark_copy(k):
        d = peer(k)
        return pltpu.make_async_remote_copy(
            src_ref=marks.at[d], dst_ref=mark_ref.at[me], send_sem=msend.at[k],
            recv_sem=mrecv.at[k], device_id=device(d), device_id_type=MESH)

    def patch_copy(k):
        d = peer(k)
        return pltpu.make_async_remote_copy(
            src_ref=sent.at[d], dst_ref=got_ref.at[me], send_sem=psend.at[k],
            recv_sem=precv.at[k], device_id=device(d), device_id_type=MESH)

    def start_mark(k, carry):
        mark_copy(k).start()
        return carry

    lax.fori_loop(0, others, start_mark, 0)
    mark_ref[me] = marks[me]

    for copy in level_copies:
        copy.wait()

    scale = {(0, 0): jnp.where(own > 0.5, RESCALE, 1.0)}
    for n, key in enumerate(AROUND):
        scale[key] = jnp.where(lv[n] > 0.5, RESCALE, 1.0)
    patch_scale = {}
    for dx in (-1, 0, 1):
        patch_scale[dx, 0] = scale[dx, 0]
        patch_scale[dx, 1] = jnp.concatenate([scale[dx, 0][1:], scale[dx, 1][:1]], axis=0)
        patch_scale[dx, -1] = jnp.concatenate([scale[dx, -1][-1:], scale[dx, 0][:-1]], axis=0)
    gain = jnp.where(own > 0.5, (1.0 - 1.0 / TAU_FINE) / RESCALE, 1.0 - 1.0 / TAU_COARSE)

    def target_scale(dx, dy, dz):
        value = patch_scale[dx, dy]
        return pltpu.roll(value, (-dz) % 8, axis=1) if dz else value

    shape = (SPAN_PATCHES, 8, LANES)
    lane = lax.broadcasted_iota(jnp.int32, shape, 2)
    for q in range(1, 19):
        e = VELOCITIES[q]
        kinds = [{}]
        for axis in range(3):
            if e[axis]:
                kinds = [{**k, axis: v} for k in kinds for v in (0, 1)]
        table = [(k, target_scale(*[e[a] * k.get(a, 0) for a in range(3)])) for k in kinds]
        for tile in range(TILES):
            cell = lane + tile * LANES
            coord = (cell // 64, (cell // 8) % 8, cell % 8)
            result = table[0][1]
            for k, value in table[1:]:
                mask = None
                for axis, on in k.items():
                    if on:
                        hit = coord[axis] == (7 if e[axis] == 1 else 0)
                        mask = hit if mask is None else mask & hit
                result = jnp.where(mask, value, result)
            cq[q - 1, :, :, tile * LANES : (tile + 1) * LANES] = gain * result

    full = (SPAN_PATCHES, 8, CELLS)
    cell = lax.broadcasted_iota(jnp.int32, full, 2)
    coord = (cell // 64, (cell // 8) % 8, cell % 8)
    entry = {
        (axis, e): coord[axis] == (0 if e == 1 else 7) for axis in range(3) for e in (1, -1)
    }
    half = lax.broadcasted_iota(jnp.int32, (2, 8, LANES), 2) < 64
    fine = jnp.broadcast_to(own[:, :, :1] > 0.5, full)

    def roll(v, amount):
        return pltpu.roll(v, amount % CELLS, axis=2)

    def step(s, carry):
        def first(r, tile):
            lanes = slice(tile * LANES, (tile + 1) * LANES)
            plain = jnp.where(lev_ref[r] > 0.5, 1.0 - 1.0 / TAU_FINE, 1.0 - 1.0 / TAU_COARSE)

            def put(q, value):
                pb[q, r, :, lanes] = value

            relax_into(lambda q: st[q, r, :, lanes], put,
                       lambda q: cq[q - 1, r, :, lanes] if q else plain)

        def shift_z(q, rows):
            e = VELOCITIES[q][2]
            if e:
                v = pb[q, rows]
                wrapped = pltpu.roll(roll(v, e - 8 * e), e % 8, axis=1)
                pb[q, rows] = jnp.where(entry[2, e][rows], wrapped, roll(v, e))

        def outer(m, carry):
            for tile in range(TILES):
                first(m * (SPAN_PATCHES - 1), tile)
            return carry

        lax.fori_loop(0, 2, outer, 0)
        for r in (0, SPAN_PATCHES - 1):
            for q in range(19):
                shift_z(q, slice(r, r + 1))
        for n in range(5):
            ys[s, 0, n] = pb[Y_UP[n], SPAN_PATCHES - 1]
            ys[s, 1, n] = pb[Y_DOWN[n], 0]
        y_copies = []
        for way, dy in ((0, 1), (1, -1)):
            copy = pltpu.make_async_remote_copy(
                src_ref=ys.at[s, way], dst_ref=yr.at[s, way], send_sem=send_sem.at[s, way],
                recv_sem=recv_sem.at[s, way], device_id=at(0, dy), device_id_type=MESH)
            copy.start()
            y_copies.append(copy)

        def inner(r, carry):
            for tile in range(TILES):
                first(r, tile)
            return carry

        lax.fori_loop(1, SPAN_PATCHES - 1, inner, 0)
        for q in range(19):
            shift_z(q, slice(1, SPAN_PATCHES - 1))
        st[0] = pb[0]
        st[5] = pb[5]
        st[6] = pb[6]
        def shift_x(wanted):
            for way, e, group in ((0, 1, X_UP), (1, -1, X_DOWN)):
                for n, q in enumerate(group):
                    if (VELOCITIES[q][1] != 0) != wanted:
                        continue
                    v = roll(pb[q], 64 * e)
                    pb[q] = v
                    edge = v[:, :, :LANES] if e == 1 else v[:, :, CELLS - LANES :]
                    turned = pltpu.roll(edge, 64, axis=2)
                    if e == 1:
                        xs[s, way, n] = jnp.where(half, edge[:2], turned[2:])
                    else:
                        xs[s, way, n] = jnp.where(half, turned[:2], edge[2:])

        def shift_y(wanted):
            for way, e, group in ((0, 1, Y_UP), (1, -1, Y_DOWN)):
                for n, q in enumerate(group):
                    if (VELOCITIES[q][0] != 0) != wanted:
                        continue
                    v = pb[q]
                    halo = yr[s, way, n][None]
                    if e == 1:
                        moved = jnp.concatenate([halo, v[:-1]], axis=0)
                    else:
                        moved = jnp.concatenate([v[1:], halo], axis=0)
                    v = jnp.where(entry[1, e], roll(moved, 8 * e - 64 * e), roll(v, 8 * e))
                    if wanted:
                        pb[q] = v
                    else:
                        st[q] = v

        shift_x(False)
        for copy in y_copies:
            copy.wait()
        shift_y(True)
        shift_x(True)
        x_copies = []
        for way, dx in ((0, 1), (1, -1)):
            copy = pltpu.make_async_remote_copy(
                src_ref=xs.at[s, way], dst_ref=xr.at[s, way], send_sem=send_sem.at[s, 2 + way],
                recv_sem=recv_sem.at[s, 2 + way], device_id=at(dx, 0), device_id_type=MESH)
            copy.start()
            x_copies.append(copy)
        shift_y(False)
        for q in X_UP + X_DOWN:
            st[q] = pb[q]

        def again(r, tiles):
            for tile in tiles:
                lanes = slice(tile * LANES, (tile + 1) * LANES)

                def put(q, value):
                    pb[q, r, :, lanes] = value

                relax_into(lambda q: st[q, r, :, lanes], put, lambda q: 1.0 - 1.0 / TAU_FINE)

        def middle(r, carry):
            again(r, range(1, TILES - 1))
            return carry

        lax.fori_loop(0, SPAN_PATCHES, middle, 0)
        for copy in x_copies:
            copy.wait()
        for way, e, group in ((0, 1, X_UP), (1, -1, X_DOWN)):
            outside = b == (0 if e == 1 else nb - 1)
            for n, q in enumerate(group):
                h = xr[s, way, n]
                turned = pltpu.roll(h, 64, axis=2)
                halo = jnp.concatenate([h, turned] if e == 1 else [turned, h], axis=0)
                along = e * INFLOW
                const = WEIGHTS[q] * (1.0 + 3.0 * along + 4.5 * along * along - 1.5 * INFLOW * INFLOW)
                halo = jnp.where(outside, jnp.full(halo.shape, const, jnp.float32), halo)
                if e == 1:
                    st[q, :, :, :LANES] = jnp.where(lane < 64, halo, st[q, :, :, :LANES])
                else:
                    st[q, :, :, CELLS - LANES :] = jnp.where(lane >= 64, halo, st[q, :, :, CELLS - LANES :])

        def ends(r, carry):
            again(r, (0, TILES - 1))
            return carry

        lax.fori_loop(0, SPAN_PATCHES, ends, 0)
        for q in range(19):
            e = VELOCITIES[q]
            take = fine
            for axis in range(3):
                if e[axis]:
                    take = take & ~entry[axis, e[axis]]
            moved = pb[q]
            if q:
                moved = roll(moved, 64 * e[0] + 8 * e[1] + e[2])
            st[q] = jnp.where(take, moved, st[q])
        return carry

    lax.fori_loop(0, STEPS, step, 0)

    for q in range(19):
        for r in range(SPAN_PATCHES):
            pm[r * 8 : r * 8 + 8, q, :] = st[q, r]

    def pack(d):
        for slot in range(2):
            p = sidx[2 * d + slot]
            for tile in range(TILES):
                lanes = slice(tile * LANES, (tile + 1) * LANES)
                at_row = slot * TILES + tile
                sent[d, at_row * MAIN : (at_row + 1) * MAIN, :] = pm[p, :MAIN, lanes]
                low = 2 * TILES * MAIN + at_row * TAIL
                sent[d, low : low + TAIL, :] = pm[p, MAIN:, lanes]

    def post(k, carry):
        pack(peer(k))

        @pl.when(k > 0)
        def _():
            patch_copy(k - 1).start()

        return carry

    lax.fori_loop(0, others, post, 0)
    pack(me)
    patch_copy(others - 1).start()
    got_ref[me] = sent[me]

    def marked(k, carry):
        mark_copy(k).wait()
        return carry

    lax.fori_loop(0, others, marked, 0)
    source = lax.broadcasted_iota(jnp.int32, (others + 1, LANES), 0) * 2
    wanted = lax.broadcasted_iota(jnp.int32, (others + 1, LANES), 1).astype(jnp.float32)
    index = jnp.where(mark_ref[:, 0, :] == wanted, source, 0)
    index = index + jnp.where(mark_ref[:, 1, :] == wanted, source + 1, 0)
    table_ref[...] = jnp.broadcast_to(jnp.sum(index, axis=0, keepdims=True), (8, LANES))

    def finish(k, carry):
        patch_copy(k).wait()
        return carry

    lax.fori_loop(0, others, finish, 0)


def unpack_kernel(ridx, got_ref, out_ref):
    def place(t, carry):
        a = ridx[0, t]
        src = a // 2
        slot = lax.rem(a, 2)
        tail = got_ref[src, 2 * TILES * MAIN : ROWS, :]
        for tile in range(TILES):
            lanes = slice(tile * LANES, (tile + 1) * LANES)
            low = pl.multiple_of((slot * TILES + tile) * MAIN, MAIN)
            out_ref[:MAIN, t, lanes] = got_ref[src, pl.ds(low, MAIN), :]
            other = TAIL * (TILES + tile)
            rest = jnp.where(
                slot == 0, tail[TAIL * tile : TAIL * (tile + 1)], tail[other : other + TAIL]
            )
            out_ref[MAIN:, t, lanes] = rest
        return carry

    for t in range(out_ref.shape[1]):
        place(t, 0)


def body(nb, nc, f_home, levels, plan):
    devices = nb * nc
    patches = f_home.shape[0]
    target = plan // patches
    order = jnp.arange(patches, dtype=jnp.int32)
    earlier = (target[:, None] == target[None, :]) & (order[None, :] < order[:, None])
    place = 2 * target + jnp.sum(earlier.astype(jnp.int32), axis=1)
    hit = place[None, :] == jnp.arange(2 * devices, dtype=jnp.int32)[:, None]
    sidx = jnp.sum(jnp.where(hit, order[None, :], 0), axis=1)
    slot_of = jnp.sum(jnp.where(hit, plan[None, :] % patches + 1, 0), axis=1) - 1
    vmem = pl.BlockSpec(memory_space=pltpu.VMEM)
    smem = pl.BlockSpec(memory_space=pltpu.SMEM)
    state = (19, SPAN_PATCHES, 8, CELLS)
    small = (SPAN_PATCHES, 8, LANES)
    f32 = jnp.float32
    dma = pltpu.SemaphoreType.DMA
    got, ridx = pl.pallas_call(
        lambda *refs: lattice_kernel(nb, nc, *refs),
        out_shape=(
            jax.ShapeDtypeStruct((devices, ROWS, LANES), f32),
            jax.ShapeDtypeStruct((8, LANES), jnp.int32),
        ),
        in_specs=[smem, smem, smem, vmem],
        out_specs=(vmem, vmem),
        scratch_shapes=[
            pltpu.VMEM(state, f32),
            pltpu.VMEM(state, f32),
            pltpu.VMEM((18,) + state[1:], f32),
            pltpu.VMEM((patches, 19, CELLS), f32),
            pltpu.VMEM((devices, ROWS, LANES), f32),
            pltpu.VMEM((devices, 8, LANES), f32),
            pltpu.VMEM((devices, 8, LANES), f32),
            pltpu.VMEM(small, f32),
            pltpu.VMEM((len(AROUND),) + small, f32),
            pltpu.VMEM((STEPS, 2, 5, 8, CELLS), f32),
            pltpu.VMEM((STEPS, 2, 5, 8, CELLS), f32),
            pltpu.VMEM((STEPS, 2, 5, 2, 8, LANES), f32),
            pltpu.VMEM((STEPS, 2, 5, 2, 8, LANES), f32),
            dma((STEPS, 4)),
            dma((STEPS, 4)),
            dma((len(AROUND),)),
            dma((len(AROUND),)),
            dma((devices - 1,)),
            dma((devices - 1,)),
            dma((devices - 1,)),
            dma((devices - 1,)),
        ],
        compiler_params=pltpu.CompilerParams(collective_id=0, has_side_effects=True,
                                             vmem_limit_bytes=60 * 1024 * 1024),
    )(sidx, slot_of, levels, jnp.transpose(f_home, (1, 0, 2)))
    out = pl.pallas_call(
        unpack_kernel,
        out_shape=jax.ShapeDtypeStruct((19, patches, CELLS), f32),
        in_specs=[smem, vmem],
        out_specs=vmem,
        compiler_params=pltpu.CompilerParams(vmem_limit_bytes=40 * 1024 * 1024),
    )(ridx, got)
    return jnp.transpose(out, (1, 0, 2))


def solution(mesh):
    nb, nc = mesh.shape["blocks"], mesh.shape["cross"]
    in_specs = (P(("blocks", "cross"), None, None), P(("blocks", "cross")), P(("blocks", "cross")))
    out_specs = P(("blocks", "cross"), None, None)
    return jax.shard_map(
        lambda f, l, p: body(nb, nc, f, l, p),
        mesh=mesh, in_specs=in_specs, out_specs=out_specs, check_vma=False)
```
